512 devices in a mesh: sys: 32 (over z, y_hi), mode: 8 (over y_lo, x), rank: 2 (over core).
Axes of the slice: x: 4, y: 8 (y_hi: 4, y_lo: 2; y = y_hi * 2 + y_lo), z: 8, core: 2. Of those that a mesh axis runs over, the one named last changes fastest.
Arguments:
- solution_core: bfloat16 [2048, 256, 64], P(('sys', 'rank'), 'mode'), parts along dimension 0, may hold values from -6 to 6
- operator_core: bfloat16 [256, 256, 256, 8], P('sys', 'rank', 'mode'), parts along dimension 0, may hold values from -0.125 to 0.125
- left_interface: bfloat16 [2048, 8, 64], P('sys', None, 'rank'), parts along dimension 0, may hold values from -0.25 to 0.25
- right_interface: bfloat16 [2048, 8, 16], P('sys'), parts along dimension 0, may hold values from -0.75 to 0.75
- rhs_left: bfloat16 [2048, 16], P(('sys', 'rank')), parts along dimension 0, may hold values from -1.5 to 1.5
- rhs_core: bfloat16 [512, 256, 16], P('sys', 'mode'), parts along dimension 0, may hold values from -6 to 6
- rhs_right: bfloat16 [512, 16], P('sys'), parts along dimension 0, may hold values from -1.5 to 1.5
Outputs:
- q_core: float32 [2048, 256, 80], P(('sys', 'rank'), 'mode'), parts along dimension 0
- r_factor: float32 [2560, 80], P('sys'), parts along dimension 0
The draws below stay inside these ranges and needn't reach their ends.
There are 32 independent parts, one for each index of `sys`. The reference program is written for one: setup_inputs(seed, part) draws one part's arguments, and reference() takes and returns one part's arrays. A program takes and returns all parts, laid end to end along the dimension named above; each array names one. Nothing has to cross between parts.
All inputs are finite; a program needn't handle non-finite values.
Results may differ from the reference program's by a relative error of at most 0.0014.
Values may be sent and summed in bfloat16 or wider, within the bound.
No kernel may reach another device: no remote copies, remote signals or barrier semaphores. Data moves between devices by JAX's collectives and lax.ppermute only.
A program may use at most 64 MiB of HBM per device.

```python
import jax
import jax.numpy as jnp
from jax import lax

R = 64
MODE = 256
RA = 8
RZ = 16
RF = 16
N_MODE = 8


def steps_of(rng, dims, split, least, largest):
    loudness = 1.0
    for dim, blocks in split:
        draws = jax.random.uniform(jax.random.fold_in(jax.random.fold_in(rng, 6), dim), (blocks,), jnp.float32, least / len(split), largest / len(split))
        loudness = loudness * jnp.repeat(jnp.exp(draws), dims[dim] // blocks).reshape((-1,) + (1,) * (len(dims) - 1 - dim))
    return loudness


def normal_values(key, extent, scale, bound, shards=(), held_as=jnp.bfloat16):
    values = jax.random.normal(key, extent, jnp.float32) * scale
    if len(shards) > 0:
        values = steps_of(key, extent, shards, -0.22, 0.18) * values
    return jnp.clip(values, min=-bound, max=bound).astype(held_as)


def setup_inputs(seed: int = 0, part: int = 0) -> dict:
    streams_of = jax.random.split(jax.random.key(seed), 8)
    own_keys = jax.random.split(jax.random.fold_in(streams_of[7], part), 8)
    return {
        "solution_core": normal_values(own_keys[0], (R, MODE, R), 1.0, 6.0, ((0, 2), (1, 8))),
        "operator_core": normal_values(own_keys[1], (RA, MODE, MODE, RA), (MODE * RA) ** -0.5, 0.125, ((1, 2), (2, 8))),
        "left_interface": normal_values(own_keys[2], (R, RA, R), (R * RA) ** -0.5, 0.25, ((2, 2),)),
        "right_interface": normal_values(own_keys[3], (R, RA, RZ), R ** -0.5, 0.75),
        "rhs_left": normal_values(own_keys[4], (R, RF), RF ** -0.5, 1.5, ((0, 2),)),
        "rhs_core": normal_values(own_keys[5], (RF, MODE, RF), 1.0, 6.0, ((1, 8),)),
        "rhs_right": normal_values(own_keys[6], (RF, RZ), RF ** -0.5, 1.5),
    }


def reference(solution_core, operator_core, left_interface, right_interface, rhs_left, rhs_core, rhs_right):
    f32 = jnp.float32
    projected = jnp.einsum('cjd,dyb->cjyb', solution_core.astype(f32), right_interface.astype(f32)).astype(jnp.bfloat16)
    width = MODE // N_MODE
    operator_term = jnp.zeros((R, MODE, RZ), f32)
    for block in range(N_MODE):
        ops = operator_core[:, :, block * width:(block + 1) * width, :].astype(f32)
        proj = projected[:, block * width:(block + 1) * width].astype(f32)
        applied = jnp.einsum('xijy,cjyb->cxib', ops, proj).astype(jnp.bfloat16)
        operator_term = operator_term + jnp.einsum('axc,cxib->aib', left_interface.astype(f32), applied.astype(f32))
    rhs_term = jnp.einsum('af,fig,gb->aib', rhs_left.astype(f32), rhs_core.astype(f32), rhs_right.astype(f32), precision=lax.Precision.HIGHEST)
    residual_core = rhs_term - operator_term
    enriched = jnp.concatenate([solution_core.astype(f32), residual_core], axis=2).reshape(R * MODE, R + RZ)
    gram = jnp.dot(enriched.T, enriched, precision=lax.Precision.HIGHEST)
    lower = jnp.linalg.cholesky(gram)
    solved = lax.linalg.triangular_solve(lower, enriched, left_side=False, lower=True, transpose_a=True)
    q_core = solved.reshape(R, MODE, R + RZ)
    return (q_core, lower.T)
```

```python
import jax
import jax.numpy as jnp
from jax import lax
from jax.experimental import pallas as pl
from jax.experimental.pallas import tpu as pltpu
from jax.sharding import PartitionSpec as P

INTERPRET = False
F32 = jnp.float32
BF16 = jnp.bfloat16
HIGHEST = lax.Precision.HIGHEST

R = 64
RZ = 16
RA = 8
HALF = 32
ROWS = 1024
NT = (((1,), (1,)), ((), ()))
TN = (((0,), (0,)), ((), ()))


def call(body, outs, *args, scratch=(), flops=0, **kw):
    return pl.pallas_call(
        body,
        out_shape=outs,
        scratch_shapes=scratch,
        interpret=INTERPRET,
        cost_estimate=pl.CostEstimate(flops=flops, bytes_accessed=1 << 20, transcendentals=0),
        **kw,
    )(*args)


def three_parts(x):
    hi = x.astype(BF16)
    rest = x - hi.astype(F32)
    mid = rest.astype(BF16)
    return hi, mid, (rest - mid.astype(F32)).astype(BF16)


def project(both_ref, right_ref, proj_ref, left_ref, gram_ref, sol_ref):
    sol_ref[0:ROWS] = both_ref[0, 0:ROWS].astype(F32)
    sol_ref[ROWS : 2 * ROWS] = both_ref[1, 0:ROWS].astype(F32)
    right = right_ref[...]
    for j in range(32):
        rows = sol_ref[pl.ds(j, R, stride=32), :].astype(BF16)
        proj_ref[j] = lax.dot_general(right, rows, NT, preferred_element_type=F32).astype(BF16)
    for x in range(RA):
        for r in range(2):
            left_ref[x, HALF * r : HALF * (r + 1)] = both_ref[r, ROWS + HALF * x : ROWS + HALF * (x + 1)]
    gram = jnp.zeros((R, R), F32)
    for r in range(2):
        s = both_ref[r, 0:ROWS]
        gram = gram + lax.dot_general(s, s, TN, preferred_element_type=F32)
    for p, part in enumerate(three_parts(gram)):
        part = part.astype(F32)
        gram_ref[HALF * p : HALF * (p + 1)] = jnp.concatenate([part[:HALF], part[HALF:]], axis=1).astype(BF16)


def pack(part_ref, out_ref):
    for half in range(2):
        for g in range(4):
            four = [part_ref[4 * g + k, HALF * half : HALF * (half + 1), :].astype(F32) for k in range(4)]
            for q in range(4):
                piece = jnp.concatenate([x[:, 32 * q : 32 * (q + 1)] for x in four], axis=1)
                out_ref[half, q, HALF * g : HALF * (g + 1)] = piece.astype(BF16)


def residual(recv_ref, rhs_ref, sol_ref, turned_ref, send_ref, gram_ref, rows_ref):
    total = recv_ref[0].astype(F32)
    for m in range(1, 8):
        total = total + recv_ref[m].astype(F32)
    packed = total[128:160] + total[160:192] + total[192:224]
    gram_ref[0:HALF] = packed[:, 0:R]
    gram_ref[HALF:R] = packed[:, R:]
    resid = rhs_ref[...] - total[0:128]
    for k in range(4):
        shifted = resid if k == 0 else pltpu.roll(resid, 128 - 32 * k, 1)
        for g in range(4):
            b = 4 * g + k
            rows_ref[HALF * b : HALF * (b + 1)] = shifted[HALF * g : HALF * (g + 1)]
    for t in range(8):
        four = [rows_ref[pl.ds(4 * t + s, RZ, stride=32), :] for s in range(4)]
        turned_ref[:, 128 * t : 128 * (t + 1)] = jnp.concatenate([x[:, :32] for x in four], axis=1)
    turned = turned_ref[...]
    stacked = jnp.concatenate(three_parts(turned), axis=0)
    cross = jnp.dot(stacked, sol_ref[...], preferred_element_type=F32)
    cross = cross[0:16] + cross[16:32] + cross[32:48]
    own = lax.dot_general(turned, turned, NT, precision=HIGHEST, preferred_element_type=F32)
    row = jnp.concatenate([cross, own, jnp.zeros((RZ, 48), F32)], axis=1)
    for k in range(16):
        send_ref[k] = row


def eliminate(m, n):
    index = lax.broadcasted_iota(jnp.int32, (n, 1), 0)
    for k in range(n):
        row = m[k : k + 1]
        factor = jnp.where(index > k, m[:, k : k + 1] / m[k : k + 1, k : k + 1], 0.0)
        m = m - factor * row
    lane = lax.broadcasted_iota(jnp.int32, m.shape, 1)
    pivot = jnp.sum(jnp.where(lane == index, m, 0.0), axis=1, keepdims=True)
    return m * lax.rsqrt(pivot)


def first_block(gram_ref, sol_ref, turned_ref, both_ref, rows_ref):
    eye = (lax.broadcasted_iota(jnp.int32, (R, R), 0) == lax.broadcasted_iota(jnp.int32, (R, R), 1)).astype(F32)
    both = eliminate(jnp.concatenate([gram_ref[...], eye], axis=1), R)
    both_ref[...] = both
    inverse = both[:, R:]
    ortho = lax.dot_general(sol_ref[...].astype(F32), inverse, NT, precision=HIGHEST, preferred_element_type=F32)
    rows_ref[...] = jnp.concatenate([ortho, turned_ref[...].T], axis=1)


def last_block(recv_ref, both_ref, rows_ref, q_ref, r_ref):
    total = recv_ref[0]
    for k in range(1, 16):
        total = total + recv_ref[k]
    both = both_ref[...]
    cross = lax.dot_general(total[:, :R], both[:, R:], NT, precision=HIGHEST, preferred_element_type=F32)
    schur = total[:, R : R + RZ] - lax.dot_general(cross, cross, NT, precision=HIGHEST, preferred_element_type=F32)
    eye = (lax.broadcasted_iota(jnp.int32, (RZ, RZ), 0) == lax.broadcasted_iota(jnp.int32, (RZ, RZ), 1)).astype(F32)
    last = eliminate(jnp.concatenate([schur, eye], axis=1), RZ)
    inverse = last[:, RZ:]
    mixed = jnp.dot(inverse, cross, precision=HIGHEST, preferred_element_type=F32)
    eye = (lax.broadcasted_iota(jnp.int32, (R, R + RZ), 0) == lax.broadcasted_iota(jnp.int32, (R, R + RZ), 1)).astype(F32)
    weight = jnp.concatenate([eye, jnp.concatenate([-mixed, inverse], axis=1)], axis=0)
    q_ref[...] = lax.dot_general(rows_ref[...], weight, NT, precision=HIGHEST, preferred_element_type=F32)
    r_ref[0:R] = jnp.concatenate([both[:, :R], cross.T], axis=1)
    r_ref[R:] = jnp.concatenate([jnp.zeros((RZ, R), F32), last[:, :RZ]], axis=1)


def per_device(solution_core, operator_core, left_interface, right_interface, rhs_left, rhs_core, rhs_right):
    shape = jax.ShapeDtypeStruct
    sol = solution_core.reshape(ROWS, R)
    left = jnp.transpose(left_interface, (1, 2, 0)).reshape(RA * HALF, R)
    both = lax.all_gather(jnp.concatenate([sol, left], axis=0), "rank", axis=0)
    right = jnp.transpose(right_interface, (1, 2, 0)).reshape(RA * RZ, R)
    proj, left, early = call(
        project,
        (shape((32, 128, R), BF16), shape((RA, R, R), BF16), shape((96, 128), BF16)),
        both,
        right,
        scratch=[pltpu.VMEM((2 * ROWS, R), F32)],
        flops=1 << 26,
    )
    proj = jnp.transpose(proj.reshape(32, RA, RZ, R), (3, 0, 1, 2))
    left = jnp.transpose(left, (1, 0, 2))
    applied = jnp.einsum("xijy,cjyb->cxib", operator_core, proj, preferred_element_type=F32).astype(BF16)
    partial_value = jnp.einsum("cxa,cxib->aib", left, applied, preferred_element_type=F32)
    partial_value = jnp.transpose(partial_value, (2, 0, 1)).astype(BF16)
    packed = call(pack, shape((2, 4, 128, 128), BF16), partial_value, flops=1 << 24)
    everyone = lax.all_gather(packed, "rank", axis=0)
    mine = lax.dynamic_index_in_dim(everyone, lax.axis_index("rank"), axis=1, keepdims=False)
    send = jnp.concatenate(
        [mine.reshape(8, 128, 128), jnp.broadcast_to(early[None], (8, 96, 128))], axis=1
    )
    recv = lax.all_to_all(send, "mode", split_axis=0, concat_axis=0, tiled=True)
    rhs_term = jnp.einsum(
        "af,fig,gb->aib", rhs_left.astype(F32), rhs_core.astype(F32), rhs_right.astype(F32), precision=HIGHEST
    )
    rhs_term = jnp.transpose(rhs_term.reshape(HALF, 32, 4, 4), (2, 0, 3, 1)).reshape(128, 128)
    turned, send, gram = call(
        residual,
        (shape((RZ, ROWS), F32), shape((16, RZ, 128), F32), shape((R, R), F32)),
        recv,
        rhs_term,
        sol,
        scratch=[pltpu.VMEM((512, 128), F32)],
        flops=1 << 24,
    )
    recv = lax.all_to_all(send, ("mode", "rank"), split_axis=0, concat_axis=0, tiled=True)
    factor, rows = call(
        first_block,
        (shape((R, 2 * R), F32), shape((ROWS, R + RZ), F32)),
        gram,
        sol,
        turned,
        flops=1 << 32,
    )
    q_core, r_factor = call(
        last_block,
        (shape((ROWS, R + RZ), F32), shape((R + RZ, R + RZ), F32)),
        recv,
        factor,
        rows,
        flops=1 << 26,
    )
    return (q_core.reshape(HALF, 32, R + RZ), r_factor)


def solution(mesh):
    in_specs = (
        P(("sys", "rank"), "mode", None),
        P("sys", "rank", "mode", None),
        P("sys", None, "rank"),
        P("sys", None, None),
        P(("sys", "rank"), None),
        P("sys", "mode", None),
        P("sys", None),
    )
    out_specs = (P(("sys", "rank"), "mode", None), P("sys", None))
    return jax.shard_map(per_device, mesh=mesh, in_specs=in_specs, out_specs=out_specs, check_vma=False)
```

```python
import jax
import jax.numpy as jnp
from jax import lax
from jax.experimental import pallas as pl
from jax.experimental.pallas import tpu as pltpu
from jax.sharding import PartitionSpec as P

INTERPRET = False
F32 = jnp.float32
BF16 = jnp.bfloat16
HIGHEST = lax.Precision.HIGHEST

R = 64
RZ = 16
RA = 8
HALF = 32
ROWS = 1024
NT = (((1,), (1,)), ((), ()))
TN = (((0,), (0,)), ((), ()))


def call(body, outs, *args, scratch=(), flops=0, **kw):
    return pl.pallas_call(
        body,
        out_shape=outs,
        scratch_shapes=scratch,
        interpret=INTERPRET,
        compiler_params=pltpu.CompilerParams(vmem_limit_bytes=12 << 20),
        in_specs=[pl.BlockSpec(memory_space=pltpu.VMEM)] * len(args),
        out_specs=jax.tree.map(lambda _: pl.BlockSpec(memory_space=pltpu.VMEM), outs),
        cost_estimate=pl.CostEstimate(flops=flops, bytes_accessed=1 << 20, transcendentals=0),
        **kw,
    )(*args)


def three_parts(x):
    hi = x.astype(BF16)
    rest = x - hi.astype(F32)
    mid = rest.astype(BF16)
    return hi, mid, (rest - mid.astype(F32)).astype(BF16)


def project(both_ref, right_ref, proj_ref, left_ref, gram_ref, sol_ref):
    sol_ref[0:ROWS] = both_ref[0, 0:ROWS].astype(F32)
    sol_ref[ROWS : 2 * ROWS] = both_ref[1, 0:ROWS].astype(F32)
    right = right_ref[...]
    for j in range(32):
        rows = sol_ref[pl.ds(j, R, stride=32), :].astype(BF16)
        proj_ref[j] = lax.dot_general(right, rows, NT, preferred_element_type=F32).astype(BF16)
    for x in range(RA):
        for r in range(2):
            left_ref[x, HALF * r : HALF * (r + 1)] = both_ref[r, ROWS + HALF * x : ROWS + HALF * (x + 1)]
    gram = jnp.zeros((R, R), F32)
    for r in range(2):
        s = both_ref[r, 0:ROWS]
        gram = gram + lax.dot_general(s, s, TN, preferred_element_type=F32)
    for p, part in enumerate(three_parts(gram)):
        part = part.astype(F32)
        gram_ref[HALF * p : HALF * (p + 1)] = jnp.concatenate([part[:HALF], part[HALF:]], axis=1).astype(BF16)


def pack(part_ref, out_ref):
    for half in range(2):
        for g in range(4):
            four = [part_ref[4 * g + k, HALF * half : HALF * (half + 1), :].astype(F32) for k in range(4)]
            for q in range(4):
                piece = jnp.concatenate([x[:, 32 * q : 32 * (q + 1)] for x in four], axis=1)
                out_ref[half, q, HALF * g : HALF * (g + 1)] = piece.astype(BF16)


def residual(recv_ref, rhs_ref, sol_ref, turned_ref, send_ref, gram_ref, rows_ref):
    total = recv_ref[0].astype(F32)
    for m in range(1, 8):
        total = total + recv_ref[m].astype(F32)
    packed = total[128:160] + total[160:192] + total[192:224]
    gram_ref[0:HALF] = packed[:, 0:R]
    gram_ref[HALF:R] = packed[:, R:]
    resid = rhs_ref[...] - total[0:128]
    for k in range(4):
        shifted = resid if k == 0 else pltpu.roll(resid, 128 - 32 * k, 1)
        for g in range(4):
            b = 4 * g + k
            rows_ref[HALF * b : HALF * (b + 1)] = shifted[HALF * g : HALF * (g + 1)]
    for t in range(8):
        four = [rows_ref[pl.ds(4 * t + s, RZ, stride=32), :] for s in range(4)]
        turned_ref[:, 128 * t : 128 * (t + 1)] = jnp.concatenate([x[:, :32] for x in four], axis=1)
    turned = turned_ref[...]
    stacked = jnp.concatenate(three_parts(turned), axis=0)
    cross = jnp.dot(stacked, sol_ref[...], preferred_element_type=F32)
    cross = cross[0:16] + cross[16:32] + cross[32:48]
    own = lax.dot_general(turned, turned, NT, precision=HIGHEST, preferred_element_type=F32)
    row = jnp.concatenate([cross, own, jnp.zeros((RZ, 48), F32)], axis=1)
    for k in range(16):
        send_ref[k] = row


def eliminate(m, n):
    index = lax.broadcasted_iota(jnp.int32, (n, 1), 0)
    for k in range(n):
        row = m[k : k + 1]
        factor = jnp.where(index > k, m[:, k : k + 1] / m[k : k + 1, k : k + 1], 0.0)
        m = m - factor * row
    lane = lax.broadcasted_iota(jnp.int32, m.shape, 1)
    pivot = jnp.sum(jnp.where(lane == index, m, 0.0), axis=1, keepdims=True)
    return m * lax.rsqrt(pivot)


def first_block(gram_ref, sol_ref, turned_ref, both_ref, rows_ref):
    eye = (lax.broadcasted_iota(jnp.int32, (R, R), 0) == lax.broadcasted_iota(jnp.int32, (R, R), 1)).astype(F32)
    both = eliminate(jnp.concatenate([gram_ref[...], eye], axis=1), R)
    both_ref[...] = both
    inverse = both[:, R:]
    ortho = lax.dot_general(sol_ref[...].astype(F32), inverse, NT, precision=HIGHEST, preferred_element_type=F32)
    rows_ref[...] = jnp.concatenate([ortho, turned_ref[...].T], axis=1)


def last_block(recv_ref, both_ref, rows_ref, q_ref, r_ref):
    total = recv_ref[0]
    for k in range(1, 16):
        total = total + recv_ref[k]
    both = both_ref[...]
    cross = lax.dot_general(total[:, :R], both[:, R:], NT, precision=HIGHEST, preferred_element_type=F32)
    schur = total[:, R : R + RZ] - lax.dot_general(cross, cross, NT, precision=HIGHEST, preferred_element_type=F32)
    eye = (lax.broadcasted_iota(jnp.int32, (RZ, RZ), 0) == lax.broadcasted_iota(jnp.int32, (RZ, RZ), 1)).astype(F32)
    last = eliminate(jnp.concatenate([schur, eye], axis=1), RZ)
    inverse = last[:, RZ:]
    mixed = jnp.dot(inverse, cross, precision=HIGHEST, preferred_element_type=F32)
    eye = (lax.broadcasted_iota(jnp.int32, (R, R + RZ), 0) == lax.broadcasted_iota(jnp.int32, (R, R + RZ), 1)).astype(F32)
    weight = jnp.concatenate([eye, jnp.concatenate([-mixed, inverse], axis=1)], axis=0)
    q_ref[...] = lax.dot_general(rows_ref[...], weight, NT, precision=HIGHEST, preferred_element_type=F32)
    r_ref[0:R] = jnp.concatenate([both[:, :R], cross.T], axis=1)
    r_ref[R:] = jnp.concatenate([jnp.zeros((RZ, R), F32), last[:, :RZ]], axis=1)


def per_device(solution_core, operator_core, left_interface, right_interface, rhs_left, rhs_core, rhs_right):
    shape = jax.ShapeDtypeStruct
    sol = solution_core.reshape(ROWS, R)
    left = jnp.transpose(left_interface, (1, 2, 0)).reshape(RA * HALF, R)
    both = lax.all_gather(jnp.concatenate([sol, left], axis=0), "rank", axis=0)
    right = jnp.transpose(right_interface, (1, 2, 0)).reshape(RA * RZ, R)
    proj, left, early = call(
        project,
        (shape((32, 128, R), BF16), shape((RA, R, R), BF16), shape((96, 128), BF16)),
        both,
        right,
        scratch=[pltpu.VMEM((2 * ROWS, R), F32)],
        flops=1 << 26,
    )
    proj = jnp.transpose(proj.reshape(32, RA, RZ, R), (3, 0, 1, 2))
    left = jnp.transpose(left, (1, 0, 2))
    applied = jnp.einsum("xijy,cjyb->cxib", operator_core, proj, preferred_element_type=F32).astype(BF16)
    partial_value = jnp.einsum("cxa,cxib->aib", left, applied, preferred_element_type=F32)
    partial_value = jnp.transpose(partial_value, (2, 0, 1)).astype(BF16)
    packed = call(pack, shape((2, 4, 128, 128), BF16), partial_value, flops=1 << 24)
    everyone = lax.all_gather(packed, "rank", axis=0)
    mine = lax.dynamic_index_in_dim(everyone, lax.axis_index("rank"), axis=1, keepdims=False)
    send = jnp.concatenate(
        [mine.reshape(8, 128, 128), jnp.broadcast_to(early[None], (8, 96, 128))], axis=1
    )
    recv = lax.all_to_all(send, "mode", split_axis=0, concat_axis=0, tiled=True)
    rhs_term = jnp.einsum(
        "af,fig,gb->aib", rhs_left.astype(F32), rhs_core.astype(F32), rhs_right.astype(F32), precision=HIGHEST
    )
    rhs_term = jnp.transpose(rhs_term.reshape(HALF, 32, 4, 4), (2, 0, 3, 1)).reshape(128, 128)
    turned, send, gram = call(
        residual,
        (shape((RZ, ROWS), F32), shape((16, RZ, 128), F32), shape((R, R), F32)),
        recv,
        rhs_term,
        sol,
        scratch=[pltpu.VMEM((512, 128), F32)],
        flops=1 << 24,
    )
    recv = lax.all_to_all(send, ("mode", "rank"), split_axis=0, concat_axis=0, tiled=True)
    factor, rows = call(
        first_block,
        (shape((R, 2 * R), F32), shape((ROWS, R + RZ), F32)),
        gram,
        sol,
        turned,
        flops=1 << 32,
    )
    q_core, r_factor = call(
        last_block,
        (shape((ROWS, R + RZ), F32), shape((R + RZ, R + RZ), F32)),
        recv,
        factor,
        rows,
        flops=1 << 26,
    )
    return (q_core.reshape(HALF, 32, R + RZ), r_factor)


def solution(mesh):
    in_specs = (
        P(("sys", "rank"), "mode", None),
        P("sys", "rank", "mode", None),
        P("sys", None, "rank"),
        P("sys", None, None),
        P(("sys", "rank"), None),
        P("sys", "mode", None),
        P("sys", None),
    )
    out_specs = (P(("sys", "rank"), "mode", None), P("sys", None))
    return jax.shard_map(per_device, mesh=mesh, in_specs=in_specs, out_specs=out_specs, check_vma=False)
```

```python
import jax
import jax.numpy as jnp
from jax import lax
from jax.experimental import pallas as pl
from jax.experimental.pallas import tpu as pltpu
from jax.sharding import PartitionSpec as P

INTERPRET = False
F32 = jnp.float32
BF16 = jnp.bfloat16
HIGHEST = lax.Precision.HIGHEST

R = 64
RZ = 16
RA = 8
HALF = 32
ROWS = 1024
NT = (((1,), (1,)), ((), ()))
TN = (((0,), (0,)), ((), ()))


VMEM = pl.BlockSpec(memory_space=pltpu.VMEM)


def call(body, outs, *args, scratch=(), flops=0, in_specs=None):
    return pl.pallas_call(
        body,
        out_shape=outs,
        in_specs=in_specs or [VMEM] * len(args),
        out_specs=jax.tree.map(lambda _: VMEM, outs),
        scratch_shapes=scratch,
        interpret=INTERPRET,
        compiler_params=pltpu.CompilerParams(vmem_limit_bytes=12 << 20),
        cost_estimate=pl.CostEstimate(flops=flops, bytes_accessed=1 << 20, transcendentals=0),
    )(*args)


def in_hbm(x):
    return x if INTERPRET else pltpu.with_memory_space_constraint(x, pltpu.HBM)


def three_parts(x):
    hi = x.astype(BF16)
    rest = x - hi.astype(F32)
    mid = rest.astype(BF16)
    return hi, mid, (rest - mid.astype(F32)).astype(BF16)


def join(sol_ref, left_ref, out_ref, sem):
    copies = [
        pltpu.make_async_copy(sol_ref, out_ref.at[0:ROWS], sem.at[0]),
        pltpu.make_async_copy(left_ref, out_ref.at[ROWS : ROWS + RA * HALF], sem.at[1]),
    ]
    for copy in copies:
        copy.start()
    for copy in copies:
        copy.wait()


def same(rows, lanes, row_of, lane_of):
    row = lax.broadcasted_iota(jnp.int32, (rows, lanes), 0)
    lane = lax.broadcasted_iota(jnp.int32, (rows, lanes), 1)
    return row_of(row) == lane_of(lane)


def project(both_ref, right_ref, rhs_left_ref, rhs_core_ref, rhs_right_ref, proj_ref, left_ref, gram_ref, rhs_ref, sol_ref):
    sol_ref[0:ROWS] = both_ref[0, 0:ROWS].astype(F32)
    sol_ref[ROWS : 2 * ROWS] = both_ref[1, 0:ROWS].astype(F32)
    right = right_ref[...]
    for j in range(32):
        rows = sol_ref[pl.ds(j, R, stride=32), :].astype(BF16)
        proj_ref[j] = lax.dot_general(right, rows, NT, preferred_element_type=F32).astype(BF16)
    for x in range(RA):
        for r in range(2):
            left_ref[x, HALF * r : HALF * (r + 1)] = both_ref[r, ROWS + HALF * x : ROWS + HALF * (x + 1)]
    gram = jnp.zeros((R, R), F32)
    for r in range(2):
        s = both_ref[r, 0:ROWS]
        gram = gram + lax.dot_general(s, s, TN, preferred_element_type=F32)
    for p, part in enumerate(three_parts(gram)):
        part = part.astype(F32)
        gram_ref[HALF * p : HALF * (p + 1)] = jnp.concatenate([part[:HALF], part[HALF:]], axis=1).astype(BF16)
    group = lax.broadcasted_iota(jnp.int32, (HALF, 128), 1) >> 4
    turned = jnp.concatenate([rhs_right_ref[...].astype(F32).T] * 8, axis=1)
    turned = jnp.broadcast_to(turned[:, None, :], (16, 16, 128)).reshape(256, 128)
    row = lax.broadcasted_iota(jnp.int32, (256, 128), 0) & 15
    lane = lax.broadcasted_iota(jnp.int32, (256, 128), 1) >> 4
    spread = jnp.concatenate([jnp.where(row == lane + 8 * h, turned, 0.0) for h in range(2)], axis=1).astype(BF16)
    half_done = jnp.dot(spread, rhs_core_ref[...], preferred_element_type=F32)
    turned = jnp.concatenate([rhs_left_ref[...].astype(F32).T] * 8, axis=1)
    blank = jnp.zeros((HALF, 128), F32)
    spread = []
    for b in range(RZ):
        tile = jnp.where(group == b % 8, turned, 0.0)
        spread.append(jnp.concatenate([tile, blank] if b < 8 else [blank, tile], axis=1))
    spread = jnp.concatenate(spread, axis=0).astype(BF16)
    total = jnp.zeros((512, 32), F32)
    for part in three_parts(half_done):
        total = total + jnp.dot(spread, part, preferred_element_type=F32)
    rhs_ref[...] = total


def pack(rank_ref, part_ref, keep_ref, give_ref):
    rank = rank_ref[0]
    for out_ref, half in ((keep_ref, rank), (give_ref, 1 - rank)):
        rows = pl.ds(pl.multiple_of(HALF * half, HALF), HALF)
        for g in range(4):
            four = [part_ref[4 * g + k, rows, :].astype(F32) for k in range(4)]
            for q in range(4):
                piece = jnp.concatenate([x[:, 32 * q : 32 * (q + 1)] for x in four], axis=1)
                out_ref[q, HALF * g : HALF * (g + 1)] = piece.astype(BF16)


def choose(rank_ref, keep_ref, every_ref, gram_ref, out_ref):
    rank = rank_ref[0]
    gram = gram_ref[...]
    for q in range(4):
        out_ref[4 * rank + q, 0:128] = keep_ref[q]
        out_ref[4 - 4 * rank + q, 0:128] = every_ref[1 - rank, q]
    for k in range(8):
        out_ref[k, 128:224] = gram


def residual(recv_ref, rhs_ref, sol_ref, turned_ref, send_ref, gram_ref, rows_ref):
    total = recv_ref[0].astype(F32)
    for m in range(1, 8):
        total = total + recv_ref[m].astype(F32)
    packed = total[128:160] + total[160:192] + total[192:224]
    gram_ref[0:HALF] = packed[:, 0:R]
    gram_ref[HALF:R] = packed[:, R:]
    for k in range(4):
        shifted = total[0:128] if k == 0 else pltpu.roll(total[0:128], 128 - 32 * k, 1)
        for g in range(4):
            rows = slice(HALF * (4 * g + k), HALF * (4 * g + k + 1))
            rows_ref[rows] = rhs_ref[rows] - shifted[HALF * g : HALF * (g + 1), :32]
    for t in range(8):
        four = [rows_ref[pl.ds(4 * t + s, RZ, stride=32), :] for s in range(4)]
        turned_ref[:, 128 * t : 128 * (t + 1)] = jnp.concatenate(four, axis=1)
    turned = turned_ref[...]
    stacked = jnp.concatenate(three_parts(turned), axis=0)
    cross = jnp.dot(stacked, sol_ref[...], preferred_element_type=F32)
    cross = cross[0:16] + cross[16:32] + cross[32:48]
    own = lax.dot_general(turned, turned, NT, precision=HIGHEST, preferred_element_type=F32)
    row = jnp.concatenate([cross, own, jnp.zeros((RZ, 48), F32)], axis=1)
    for k in range(16):
        send_ref[k] = row


def eliminate(m, n):
    index = lax.broadcasted_iota(jnp.int32, (n, 1), 0)
    for k in range(n):
        row = m[k : k + 1]
        factor = jnp.where(index > k, m[:, k : k + 1] / m[k : k + 1, k : k + 1], 0.0)
        m = m - factor * row
    lane = lax.broadcasted_iota(jnp.int32, m.shape, 1)
    pivot = jnp.sum(jnp.where(lane == index, m, 0.0), axis=1, keepdims=True)
    return m * lax.rsqrt(pivot)


def first_block(gram_ref, sol_ref, both_ref, ortho_ref, parts_ref):
    eye = same(R, R, lambda r: r, lambda l: l).astype(F32)
    both = eliminate(jnp.concatenate([gram_ref[...], eye], axis=1), R)
    both_ref[...] = both
    stacked = jnp.concatenate(three_parts(both[:, R:]), axis=0)
    ortho = lax.dot_general(stacked, sol_ref[...], NT, preferred_element_type=F32)
    ortho = ortho[0:R] + ortho[R : 2 * R] + ortho[2 * R :]
    ortho_ref[...] = ortho
    hi, mid, _ = three_parts(ortho)
    for k, part in enumerate((hi, mid, hi, mid)):
        parts_ref[R * k : R * (k + 1)] = part


def last_block(recv_ref, both_ref, ortho_ref, parts_ref, turned_ref, q_ref, r_ref):
    total = recv_ref[0]
    for k in range(1, 16):
        total = total + recv_ref[k]
    both = both_ref[...]
    cross = lax.dot_general(total[:, :R], both[:, R:], NT, precision=HIGHEST, preferred_element_type=F32)
    schur = total[:, R : R + RZ] - lax.dot_general(cross, cross, NT, precision=HIGHEST, preferred_element_type=F32)
    hi, mid, _ = three_parts(cross)
    wide = jnp.concatenate([hi, hi, mid, mid], axis=1)
    resid = turned_ref[...] - jnp.dot(wide, parts_ref[...], preferred_element_type=F32)
    blocks = [resid[:, 128 * t : 128 * (t + 1)] for t in range(8)]
    columns = [jnp.broadcast_to(schur[:, k : k + 1], (RZ, 128)) for k in range(RZ)]
    index = lax.broadcasted_iota(jnp.int32, (RZ, 128), 0)
    lane = lax.broadcasted_iota(jnp.int32, (RZ, 128), 1)
    pivots = jnp.zeros((RZ, 128), F32)
    upper = jnp.zeros((RZ, 128), F32)
    for k in range(RZ):
        pivots = jnp.where(index == k, columns[k], pivots)
        upper = jnp.where((lane == R + k) & (index <= k), columns[k], upper)
        factor = jnp.where(index > k, columns[k] / columns[k][k : k + 1], 0.0)
        for j in range(k + 1, RZ):
            columns[j] = columns[j] - factor * columns[j][k : k + 1]
        blocks = [x - factor * x[k : k + 1] for x in blocks]
    scale = lax.rsqrt(pivots)
    for t in range(8):
        lanes = slice(128 * t, 128 * (t + 1))
        q_ref[lanes] = jnp.concatenate([ortho_ref[:, lanes], blocks[t] * scale], axis=0).T
    r_ref[0:R] = jnp.concatenate([both[:, :R], cross.T], axis=1)
    r_ref[R:] = (upper * scale)[:, : R + RZ]


def per_device(solution_core, operator_core, left_interface, right_interface, rhs_left, rhs_core, rhs_right):
    shape = jax.ShapeDtypeStruct
    sol = solution_core.reshape(ROWS, R)
    left = jnp.transpose(left_interface, (1, 2, 0)).reshape(RA * HALF, R)
    hbm = pl.BlockSpec(memory_space=pltpu.HBM)
    own = call(
        join,
        shape((ROWS + RA * HALF, R), BF16),
        in_hbm(sol),
        in_hbm(left),
        scratch=[pltpu.SemaphoreType.DMA((2,))],
        in_specs=[hbm, hbm],
    )
    both = lax.all_gather(own, "rank", axis=0)
    right = jnp.transpose(right_interface, (1, 2, 0)).reshape(RA * RZ, R)
    proj, left, early, rhs_term = call(
        project,
        (
            shape((32, 128, R), BF16),
            shape((RA, R, R), BF16),
            shape((96, 128), BF16),
            shape((512, 32), F32),
        ),
        both,
        right,
        rhs_left.T,
        jnp.transpose(rhs_core, (0, 2, 1)).reshape(256, 32),
        rhs_right,
        scratch=[pltpu.VMEM((2 * ROWS, R), F32)],
        flops=1 << 26,
    )
    proj = jnp.transpose(proj.reshape(32, RA, RZ, R), (3, 0, 1, 2))
    left = jnp.transpose(left, (1, 0, 2))
    applied = jnp.einsum("xijy,cjyb->cxib", operator_core, proj, preferred_element_type=F32).astype(BF16)
    partial_value = jnp.einsum("cxa,cxib->aib", left, applied, preferred_element_type=F32)
    partial_value = jnp.transpose(partial_value, (2, 0, 1)).astype(BF16)
    rank = lax.axis_index("rank").astype(jnp.int32).reshape(1)
    smem = pl.BlockSpec(memory_space=pltpu.SMEM)
    chunks = shape((4, 128, 128), BF16)
    keep, give = call(pack, (chunks, chunks), rank, partial_value, flops=1 << 24, in_specs=[smem, VMEM])
    everyone = lax.all_gather(give, "rank", axis=0)
    send = call(
        choose,
        shape((8, 224, 128), BF16),
        rank,
        keep,
        everyone,
        early,
        in_specs=[smem, VMEM, VMEM, VMEM],
    )
    recv = lax.all_to_all(send, "mode", split_axis=0, concat_axis=0, tiled=True)
    turned, send, gram = call(
        residual,
        (shape((RZ, ROWS), F32), shape((16, RZ, 128), F32), shape((R, R), F32)),
        recv,
        rhs_term,
        sol,
        scratch=[pltpu.VMEM((512, 32), F32)],
        flops=1 << 24,
    )
    recv = lax.all_to_all(send, ("mode", "rank"), split_axis=0, concat_axis=0, tiled=True)
    factor, ortho, parts = call(
        first_block,
        (shape((R, 2 * R), F32), shape((R, ROWS), F32), shape((4 * R, ROWS), BF16)),
        gram,
        sol,
        flops=1 << 32,
    )
    q_core, r_factor = call(
        last_block,
        (shape((ROWS, R + RZ), F32), shape((R + RZ, R + RZ), F32)),
        recv,
        factor,
        ortho,
        parts,
        turned,
        flops=1 << 26,
    )
    return (q_core.reshape(HALF, 32, R + RZ), r_factor)


def solution(mesh):
    in_specs = (
        P(("sys", "rank"), "mode", None),
        P("sys", "rank", "mode", None),
        P("sys", None, "rank"),
        P("sys", None, None),
        P(("sys", "rank"), None),
        P("sys", "mode", None),
        P("sys", None),
    )
    out_specs = (P(("sys", "rank"), "mode", None), P("sys", None))
    return jax.shard_map(per_device, mesh=mesh, in_specs=in_specs, out_specs=out_specs, check_vma=False)
```

```python
import jax
import jax.numpy as jnp
from jax import lax
from jax.experimental import pallas as pl
from jax.experimental.pallas import tpu as pltpu
from jax.sharding import PartitionSpec as P

INTERPRET = False
F32 = jnp.float32
BF16 = jnp.bfloat16
HIGHEST = lax.Precision.HIGHEST

R = 64
RZ = 16
RA = 8
HALF = 32
PITCH = 33
ROWS = 1024
NT = (((1,), (1,)), ((), ()))
TN = (((0,), (0,)), ((), ()))


VMEM = pl.BlockSpec(memory_space=pltpu.VMEM)


def call(body, outs, *args, scratch=(), flops=0, in_specs=None):
    return pl.pallas_call(
        body,
        out_shape=outs,
        in_specs=in_specs or [VMEM] * len(args),
        out_specs=jax.tree.map(lambda _: VMEM, outs),
        scratch_shapes=scratch,
        interpret=INTERPRET,
        compiler_params=pltpu.CompilerParams(vmem_limit_bytes=12 << 20),
        cost_estimate=pl.CostEstimate(flops=flops, bytes_accessed=1 << 20, transcendentals=0),
    )(*args)


def in_hbm(x):
    return x if INTERPRET else pltpu.with_memory_space_constraint(x, pltpu.HBM)


def three_parts(x):
    hi = x.astype(BF16)
    rest = x - hi.astype(F32)
    mid = rest.astype(BF16)
    return hi, mid, (rest - mid.astype(F32)).astype(BF16)


def join(sol_ref, left_ref, out_ref, sem):
    copies = [
        pltpu.make_async_copy(sol_ref, out_ref.at[0:ROWS], sem.at[0]),
        pltpu.make_async_copy(left_ref, out_ref.at[ROWS : ROWS + RA * HALF], sem.at[1]),
    ]
    for copy in copies:
        copy.start()
    for copy in copies:
        copy.wait()


def project(rank_ref, both_ref, right_ref, rhs_left_ref, rhs_core_ref, rhs_right_ref, proj_ref, left_ref, gram_ref, rhs_ref, sol_ref):
    for c in range(R):
        own = HALF * (c % HALF)
        sol_ref[PITCH * c : PITCH * c + 32] = both_ref[c // HALF, own : own + 32].astype(F32)
    right = right_ref[...]
    for j in range(32):
        rows = sol_ref[pl.ds(j, R, stride=PITCH), :].astype(BF16)
        proj_ref[j] = lax.dot_general(right, rows, NT, preferred_element_type=F32).astype(BF16)
    for x in range(RA):
        for r in range(2):
            left_ref[x, HALF * r : HALF * (r + 1)] = both_ref[r, ROWS + HALF * x : ROWS + HALF * (x + 1)]
    gram = jnp.zeros((R, R), F32)
    for r in range(2):
        s = both_ref[r, 0:ROWS]
        gram = gram + lax.dot_general(s, s, TN, preferred_element_type=F32)
    row = lax.broadcasted_iota(jnp.int32, (HALF, HALF), 0)
    lane = lax.broadcasted_iota(jnp.int32, (HALF, HALF), 1)
    corner = gram[HALF:, HALF:]
    half = jnp.where(rank_ref[0] == 0, jnp.where(row >= lane, gram[:HALF, :HALF], corner), gram[HALF:, :HALF])
    half = jnp.concatenate([half[8 * k : 8 * (k + 1)] for k in range(4)], axis=1)
    diagonal = jnp.sum(jnp.where(row == lane, corner, 0.0), axis=0, keepdims=True)
    diagonal = jnp.broadcast_to(jnp.concatenate([diagonal] * 4, axis=1), (8, 128))
    row = lax.broadcasted_iota(jnp.int32, (8, 128), 0)
    parts = [part.astype(F32) for part in three_parts(half)]
    tail = jnp.zeros((8, 128), F32)
    for p, part in enumerate(three_parts(diagonal)):
        tail = jnp.where(row == p, part.astype(F32), tail)
    gram_ref[...] = jnp.concatenate([*parts, tail], axis=0).astype(BF16)
    turned = jnp.concatenate([rhs_right_ref[...].astype(F32).T] * 8, axis=1)
    turned = jnp.broadcast_to(turned[:, None, :], (16, 16, 128)).reshape(256, 128)
    row = lax.broadcasted_iota(jnp.int32, (256, 128), 0) & 15
    lane = lax.broadcasted_iota(jnp.int32, (256, 128), 1) >> 4
    spread = jnp.concatenate([jnp.where(row == lane + 8 * h, turned, 0.0) for h in range(2)], axis=1).astype(BF16)
    inner = jnp.dot(spread, rhs_core_ref[...], preferred_element_type=F32)
    inner = jnp.concatenate([inner[RZ * b : RZ * (b + 1)] for b in range(RZ)], axis=1)
    stacked = jnp.concatenate(three_parts(inner), axis=0)
    outer = rhs_left_ref[...].astype(F32).T.astype(BF16)
    total = jnp.dot(jnp.concatenate([outer] * 3, axis=1), stacked, preferred_element_type=F32)
    for g in range(4):
        rhs_ref[HALF * g : HALF * (g + 1)] = total[:, 128 * g : 128 * (g + 1)]


def pack(rank_ref, part_ref, keep_ref, give_ref):
    rank = rank_ref[0]
    for out_ref, half in ((keep_ref, rank), (give_ref, 1 - rank)):
        rows = pl.ds(pl.multiple_of(HALF * half, HALF), HALF)
        for g in range(4):
            four = [part_ref[4 * g + k, rows, :].astype(F32) for k in range(4)]
            for q in range(4):
                piece = jnp.concatenate([x[:, 32 * q : 32 * (q + 1)] for x in four], axis=1)
                out_ref[q, HALF * g : HALF * (g + 1)] = piece.astype(BF16)


def choose(rank_ref, keep_ref, every_ref, gram_ref, out_ref):
    rank = rank_ref[0]
    gram = gram_ref[...]
    for q in range(4):
        out_ref[4 * rank + q, 0:128] = keep_ref[q]
        out_ref[4 - 4 * rank + q, 0:128] = every_ref[1 - rank, q]
    for k in range(8):
        out_ref[k, 128:160] = gram


def residual(recv_ref, rhs_ref, sol_ref, turned_ref, send_ref, gram_ref, rows_ref):
    total = recv_ref[0].astype(F32)
    for m in range(1, 8):
        total = total + recv_ref[m].astype(F32)
    gram_ref[0:8] = total[128:136] + total[136:144] + total[144:152]
    gram_ref[8:16] = jnp.broadcast_to(total[152:153] + total[153:154] + total[154:155], (8, 128))
    resid = rhs_ref[...] - total[0:128]
    for k in range(4):
        shifted = resid if k == 0 else pltpu.roll(resid, 128 - 32 * k, 1)
        for g in range(4):
            b = 4 * g + k
            rows_ref[PITCH * b : PITCH * b + HALF] = shifted[HALF * g : HALF * (g + 1), :32]
    for t in range(8):
        four = [rows_ref[pl.ds(4 * t + s, RZ, stride=PITCH), :] for s in range(4)]
        turned_ref[:, 128 * t : 128 * (t + 1)] = jnp.concatenate(four, axis=1)
    turned = turned_ref[...]
    stacked = jnp.concatenate(three_parts(turned), axis=0)
    cross = jnp.dot(stacked, sol_ref[...], preferred_element_type=F32)
    cross = cross[0:16] + cross[16:32] + cross[32:48]
    own = lax.dot_general(turned, turned, NT, precision=HIGHEST, preferred_element_type=F32)
    row = jnp.concatenate([cross, own, jnp.zeros((RZ, 48), F32)], axis=1)
    for k in range(16):
        send_ref[k] = row


def eliminate(square, blocks):
    columns = [jnp.broadcast_to(square[:, k : k + 1], (RZ, 128)) for k in range(RZ)]
    index = lax.broadcasted_iota(jnp.int32, (RZ, 128), 0)
    pivots = jnp.zeros((RZ, 128), F32)
    for k in range(RZ):
        pivots = jnp.where(index == k, columns[k], pivots)
        factor = jnp.where(index > k, columns[k] / columns[k][k : k + 1], 0.0)
        for j in range(k + 1, RZ):
            columns[j] = columns[j] - factor * columns[j][k : k + 1]
        blocks = [x - factor * x[k : k + 1] for x in blocks]
    return lax.rsqrt(pivots), columns, blocks


def first_block(gram_ref, sol_ref, both_ref, ortho_ref, parts_ref):
    row = lax.broadcasted_iota(jnp.int32, (HALF, HALF), 0)
    lane = lax.broadcasted_iota(jnp.int32, (HALF, HALF), 1)
    halves = [jnp.concatenate([gram_ref[r, 0:8, 32 * k : 32 * (k + 1)] for k in range(4)], axis=0) for r in range(2)]
    mirror = halves[0].T
    first = jnp.where(row >= lane, halves[0], mirror)
    corner = jnp.where(row < lane, halves[0], mirror)
    corner = jnp.where(row == lane, gram_ref[0, 8:9, 0:32], corner)
    eye = (lax.broadcasted_iota(jnp.int32, (R, R), 0) == lax.broadcasted_iota(jnp.int32, (R, R), 1)).astype(F32)
    gram = jnp.concatenate(
        [jnp.concatenate([first, halves[1].T], axis=1), jnp.concatenate([halves[1], corner], axis=1)], axis=0
    )
    rest = jnp.concatenate([gram, eye], axis=1)
    done = []
    for k in range(4):
        scale, _, (top,) = eliminate(rest[0:RZ, RZ * k : RZ * (k + 1)], [rest[0:RZ]])
        top = top * scale
        done.append(top)
        if k < 3:
            across = top[:, RZ * (k + 1) : R]
            rest = rest[RZ:] - lax.dot_general(across, top, TN, precision=HIGHEST, preferred_element_type=F32)
    both = jnp.concatenate(done, axis=0)
    both_ref[...] = both
    stacked = jnp.concatenate(three_parts(both[:, R:]), axis=0)
    ortho = lax.dot_general(stacked, sol_ref[...], NT, preferred_element_type=F32)
    ortho = ortho[0:R] + ortho[R : 2 * R] + ortho[2 * R :]
    ortho_ref[...] = ortho
    hi, mid, _ = three_parts(ortho)
    for k, part in enumerate((hi, mid, hi, mid)):
        parts_ref[R * k : R * (k + 1)] = part


def last_block(recv_ref, both_ref, ortho_ref, parts_ref, turned_ref, q_ref, r_ref):
    total = recv_ref[0]
    for k in range(1, 16):
        total = total + recv_ref[k]
    both = both_ref[...]
    cross = lax.dot_general(total[:, :R], both[:, R:], NT, precision=HIGHEST, preferred_element_type=F32)
    schur = total[:, R : R + RZ] - lax.dot_general(cross, cross, NT, precision=HIGHEST, preferred_element_type=F32)
    hi, mid, _ = three_parts(cross)
    wide = jnp.concatenate([hi, hi, mid, mid], axis=1)
    resid = turned_ref[...] - jnp.dot(wide, parts_ref[...], preferred_element_type=F32)
    blocks = [resid[:, 128 * t : 128 * (t + 1)] for t in range(8)]
    scale, columns, blocks = eliminate(schur, blocks)
    index = lax.broadcasted_iota(jnp.int32, (RZ, 128), 0)
    lane = lax.broadcasted_iota(jnp.int32, (RZ, 128), 1)
    upper = jnp.zeros((RZ, 128), F32)
    for k in range(RZ):
        upper = jnp.where((lane == R + k) & (index <= k), columns[k], upper)
    for t in range(8):
        rows = slice(128 * t, 128 * (t + 1))
        q_ref[rows] = jnp.concatenate([ortho_ref[:, rows], blocks[t] * scale], axis=0).T
    row = lax.broadcasted_iota(jnp.int32, (R, R), 0)
    lane = lax.broadcasted_iota(jnp.int32, (R, R), 1)
    r_ref[0:R] = jnp.concatenate([jnp.where(row <= lane, both[:, :R], 0.0), cross.T], axis=1)
    r_ref[R:] = (upper * scale)[:, : R + RZ]


def per_device(solution_core, operator_core, left_interface, right_interface, rhs_left, rhs_core, rhs_right):
    shape = jax.ShapeDtypeStruct
    sol = solution_core.reshape(ROWS, R)
    left = jnp.transpose(left_interface, (1, 2, 0)).reshape(RA * HALF, R)
    hbm = pl.BlockSpec(memory_space=pltpu.HBM)
    own = call(
        join,
        shape((ROWS + RA * HALF, R), BF16),
        in_hbm(sol),
        in_hbm(left),
        scratch=[pltpu.SemaphoreType.DMA((2,))],
        in_specs=[hbm, hbm],
    )
    both = lax.all_gather(own, "rank", axis=0)
    right = jnp.transpose(right_interface, (1, 2, 0)).reshape(RA * RZ, R)
    rank = lax.axis_index("rank").astype(jnp.int32).reshape(1)
    smem = pl.BlockSpec(memory_space=pltpu.SMEM)
    proj, left, early, rhs_term = call(
        project,
        (
            shape((32, 128, R), BF16),
            shape((RA, R, R), BF16),
            shape((32, 128), BF16),
            shape((128, 128), F32),
        ),
        rank,
        both,
        right,
        rhs_left.T,
        jnp.transpose(rhs_core, (0, 2, 1)).reshape(256, 32),
        rhs_right,
        scratch=[pltpu.VMEM((R * PITCH, R), F32)],
        flops=1 << 26,
        in_specs=[smem] + [VMEM] * 5,
    )
    proj = jnp.transpose(proj.reshape(32, RA, RZ, R), (3, 0, 1, 2))
    left = jnp.transpose(left, (1, 0, 2))
    applied = jnp.einsum("xijy,cjyb->cxib", operator_core, proj, preferred_element_type=F32).astype(BF16)
    partial_value = jnp.einsum("cxa,cxib->aib", left, applied, preferred_element_type=F32)
    partial_value = jnp.transpose(partial_value, (2, 0, 1)).astype(BF16)
    chunks = shape((4, 128, 128), BF16)
    keep, give = call(pack, (chunks, chunks), rank, partial_value, flops=1 << 24, in_specs=[smem, VMEM])
    everyone = lax.all_gather(give, "rank", axis=0)
    send = call(
        choose,
        shape((8, 160, 128), BF16),
        rank,
        keep,
        everyone,
        early,
        in_specs=[smem, VMEM, VMEM, VMEM],
    )
    recv = lax.all_to_all(send, "mode", split_axis=0, concat_axis=0, tiled=True)
    turned, send, gram = call(
        residual,
        (shape((RZ, ROWS), F32), shape((16, RZ, 128), F32), shape((16, 128), F32)),
        recv,
        rhs_term,
        sol,
        scratch=[pltpu.VMEM((RZ * PITCH, 32), F32)],
        flops=1 << 24,
    )
    recv = lax.all_to_all(send, ("mode", "rank"), split_axis=0, concat_axis=0, tiled=True)
    gram = lax.all_gather(gram, "rank", axis=0)
    factor, ortho, parts = call(
        first_block,
        (shape((R, 2 * R), F32), shape((R, ROWS), F32), shape((4 * R, ROWS), BF16)),
        gram,
        sol,
        flops=1 << 32,
    )
    q_core, r_factor = call(
        last_block,
        (shape((ROWS, R + RZ), F32), shape((R + RZ, R + RZ), F32)),
        recv,
        factor,
        ortho,
        parts,
        turned,
        flops=1 << 26,
    )
    return (q_core.reshape(HALF, 32, R + RZ), r_factor)


def solution(mesh):
    in_specs = (
        P(("sys", "rank"), "mode", None),
        P("sys", "rank", "mode", None),
        P("sys", None, "rank"),
        P("sys", None, None),
        P(("sys", "rank"), None),
        P("sys", "mode", None),
        P("sys", None),
    )
    out_specs = (P(("sys", "rank"), "mode", None), P("sys", None))
    return jax.shard_map(per_device, mesh=mesh, in_specs=in_specs, out_specs=out_specs, check_vma=False)
```

```python
import jax
import jax.numpy as jnp
from jax import lax
from jax.experimental import pallas as pl
from jax.experimental.pallas import tpu as pltpu
from jax.sharding import PartitionSpec as P

INTERPRET = False
F32 = jnp.float32
BF16 = jnp.bfloat16
HIGHEST = lax.Precision.HIGHEST

R = 64
RZ = 16
RA = 8
HALF = 32
PITCH = 33
ROWS = 1024
NT = (((1,), (1,)), ((), ()))
TN = (((0,), (0,)), ((), ()))


VMEM = pl.BlockSpec(memory_space=pltpu.VMEM)


def call(body, outs, *args, scratch=(), flops=0, in_specs=None):
    return pl.pallas_call(
        body,
        out_shape=outs,
        in_specs=in_specs or [VMEM] * len(args),
        out_specs=jax.tree.map(lambda _: VMEM, outs),
        scratch_shapes=scratch,
        interpret=INTERPRET,
        compiler_params=pltpu.CompilerParams(vmem_limit_bytes=12 << 20),
        cost_estimate=pl.CostEstimate(flops=flops, bytes_accessed=1 << 20, transcendentals=0),
    )(*args)


def in_hbm(x):
    return x if INTERPRET else pltpu.with_memory_space_constraint(x, pltpu.HBM)


def three_parts(x):
    hi = x.astype(BF16)
    rest = x - hi.astype(F32)
    mid = rest.astype(BF16)
    return hi, mid, (rest - mid.astype(F32)).astype(BF16)


def join(sol_ref, left_ref, out_ref, sem):
    copies = [
        pltpu.make_async_copy(sol_ref, out_ref.at[0:ROWS], sem.at[0]),
        pltpu.make_async_copy(left_ref, out_ref.at[ROWS : ROWS + RA * HALF], sem.at[1]),
    ]
    for copy in copies:
        copy.start()
    for copy in copies:
        copy.wait()


def project(rank_ref, both_ref, right_ref, rhs_left_ref, rhs_core_ref, rhs_right_ref, proj_ref, left_ref, gram_ref, rhs_ref, sol_ref):
    for c in range(R):
        own = HALF * (c % HALF)
        sol_ref[PITCH * c : PITCH * c + 32] = both_ref[c // HALF, own : own + 32].astype(F32)
    right = right_ref[...]
    for j in range(32):
        rows = sol_ref[pl.ds(j, R, stride=PITCH), :].astype(BF16)
        proj_ref[j] = lax.dot_general(right, rows, NT, preferred_element_type=F32).astype(BF16)
    for x in range(RA):
        for r in range(2):
            left_ref[x, HALF * r : HALF * (r + 1)] = both_ref[r, ROWS + HALF * x : ROWS + HALF * (x + 1)]
    gram = jnp.zeros((R, R), F32)
    for r in range(2):
        s = both_ref[r, 0:ROWS]
        gram = gram + lax.dot_general(s, s, TN, preferred_element_type=F32)
    row = lax.broadcasted_iota(jnp.int32, (HALF, HALF), 0)
    lane = lax.broadcasted_iota(jnp.int32, (HALF, HALF), 1)
    corner = gram[HALF:, HALF:]
    half = jnp.where(rank_ref[0] == 0, jnp.where(row >= lane, gram[:HALF, :HALF], corner), gram[HALF:, :HALF])
    half = jnp.concatenate([half[8 * k : 8 * (k + 1)] for k in range(4)], axis=1)
    diagonal = jnp.sum(jnp.where(row == lane, corner, 0.0), axis=0, keepdims=True)
    diagonal = jnp.broadcast_to(jnp.concatenate([diagonal] * 4, axis=1), (8, 128))
    row = lax.broadcasted_iota(jnp.int32, (8, 128), 0)
    parts = [part.astype(F32) for part in three_parts(half)]
    tail = jnp.zeros((8, 128), F32)
    for p, part in enumerate(three_parts(diagonal)):
        tail = jnp.where(row == p, part.astype(F32), tail)
    gram_ref[...] = jnp.concatenate([*parts, tail], axis=0).astype(BF16)
    turned = jnp.concatenate([rhs_right_ref[...].astype(F32).T] * 8, axis=1)
    turned = jnp.broadcast_to(turned[:, None, :], (16, 16, 128)).reshape(256, 128)
    row = lax.broadcasted_iota(jnp.int32, (256, 128), 0) & 15
    lane = lax.broadcasted_iota(jnp.int32, (256, 128), 1) >> 4
    spread = jnp.concatenate([jnp.where(row == lane + 8 * h, turned, 0.0) for h in range(2)], axis=1).astype(BF16)
    inner = jnp.dot(spread, rhs_core_ref[...], preferred_element_type=F32)
    inner = jnp.concatenate([inner[RZ * b : RZ * (b + 1)] for b in range(RZ)], axis=1)
    stacked = jnp.concatenate(three_parts(inner), axis=0)
    outer = rhs_left_ref[...].astype(F32).T.astype(BF16)
    total = jnp.dot(jnp.concatenate([outer] * 3, axis=1), stacked, preferred_element_type=F32)
    for g in range(4):
        rhs_ref[HALF * g : HALF * (g + 1)] = total[:, 128 * g : 128 * (g + 1)]


def pack(rank_ref, part_ref, keep_ref, give_ref):
    rank = rank_ref[0]
    for out_ref, half in ((keep_ref, rank), (give_ref, 1 - rank)):
        rows = pl.ds(pl.multiple_of(HALF * half, HALF), HALF)
        for g in range(4):
            four = [part_ref[4 * g + k, rows, :].astype(F32) for k in range(4)]
            for q in range(4):
                piece = jnp.concatenate([x[:, 32 * q : 32 * (q + 1)] for x in four], axis=1)
                out_ref[q, HALF * g : HALF * (g + 1)] = piece.astype(BF16)


def choose(rank_ref, keep_ref, every_ref, gram_ref, out_ref):
    rank = rank_ref[0]
    gram = gram_ref[...]
    for q in range(4):
        out_ref[4 * rank + q, 0:128] = keep_ref[q]
        out_ref[4 - 4 * rank + q, 0:128] = every_ref[1 - rank, q]
    for k in range(8):
        out_ref[k, 128:160] = gram


def residual(recv_ref, rhs_ref, sol_ref, turned_ref, send_ref, gram_ref, rows_ref):
    total = recv_ref[0].astype(F32)
    for m in range(1, 8):
        total = total + recv_ref[m].astype(F32)
    gram_ref[0:8] = total[128:136] + total[136:144] + total[144:152]
    gram_ref[8:16] = jnp.broadcast_to(total[152:153] + total[153:154] + total[154:155], (8, 128))
    resid = rhs_ref[...] - total[0:128]
    for k in range(4):
        shifted = resid if k == 0 else pltpu.roll(resid, 128 - 32 * k, 1)
        for g in range(4):
            b = 4 * g + k
            rows_ref[PITCH * b : PITCH * b + HALF] = shifted[HALF * g : HALF * (g + 1), :32]
    for t in range(8):
        four = [rows_ref[pl.ds(4 * t + s, RZ, stride=PITCH), :] for s in range(4)]
        turned_ref[:, 128 * t : 128 * (t + 1)] = jnp.concatenate(four, axis=1)
    turned = turned_ref[...]
    stacked = jnp.concatenate(three_parts(turned), axis=0)
    cross = jnp.dot(stacked, sol_ref[...], preferred_element_type=F32)
    cross = cross[0:16] + cross[16:32] + cross[32:48]
    pairs = lax.dot_general(stacked, stacked, NT, preferred_element_type=F32)
    own = pairs[0:16, 16:32] + pairs[0:16, 32:48] + pairs[16:32, 16:32] + pairs[16:32, 0:16] + pairs[32:48, 0:16]
    own = own + pairs[0:16, 0:16]
    row = jnp.concatenate([cross, own, jnp.zeros((RZ, 48), F32)], axis=1)
    for k in range(16):
        send_ref[k] = row


def eliminate(square, blocks):
    columns = [jnp.broadcast_to(square[:, k : k + 1], (RZ, 128)) for k in range(RZ)]
    index = lax.broadcasted_iota(jnp.int32, (RZ, 128), 0)
    pivots = jnp.zeros((RZ, 128), F32)
    for k in range(RZ):
        pivots = jnp.where(index == k, columns[k], pivots)
        factor = jnp.where(index > k, columns[k] / columns[k][k : k + 1], 0.0)
        for j in range(k + 1, RZ):
            columns[j] = columns[j] - factor * columns[j][k : k + 1]
        blocks = [x - factor * x[k : k + 1] for x in blocks]
    return lax.rsqrt(pivots), columns, blocks


def first_block(gram_ref, sol_ref, both_ref, ortho_ref, parts_ref):
    row = lax.broadcasted_iota(jnp.int32, (HALF, HALF), 0)
    lane = lax.broadcasted_iota(jnp.int32, (HALF, HALF), 1)
    halves = [jnp.concatenate([gram_ref[r, 0:8, 32 * k : 32 * (k + 1)] for k in range(4)], axis=0) for r in range(2)]
    mirror = halves[0].T
    first = jnp.where(row >= lane, halves[0], mirror)
    corner = jnp.where(row < lane, halves[0], mirror)
    corner = jnp.where(row == lane, gram_ref[0, 8:9, 0:32], corner)
    eye = (lax.broadcasted_iota(jnp.int32, (R, R), 0) == lax.broadcasted_iota(jnp.int32, (R, R), 1)).astype(F32)
    gram = jnp.concatenate(
        [jnp.concatenate([first, halves[1].T], axis=1), jnp.concatenate([halves[1], corner], axis=1)], axis=0
    )
    rest = jnp.concatenate([gram, eye], axis=1)
    done = []
    for k in range(4):
        scale, _, (top,) = eliminate(rest[0:RZ, RZ * k : RZ * (k + 1)], [rest[0:RZ]])
        top = top * scale
        done.append(top)
        if k < 3:
            across = top[:, RZ * (k + 1) : R]
            rest = rest[RZ:] - lax.dot_general(across, top, TN, precision=HIGHEST, preferred_element_type=F32)
    both = jnp.concatenate(done, axis=0)
    both_ref[...] = both
    stacked = jnp.concatenate(three_parts(both[:, R:]), axis=0)
    ortho = lax.dot_general(stacked, sol_ref[...], NT, preferred_element_type=F32)
    ortho = ortho[0:R] + ortho[R : 2 * R] + ortho[2 * R :]
    ortho_ref[...] = ortho
    hi, mid, _ = three_parts(ortho)
    for k, part in enumerate((hi, mid, hi, mid)):
        parts_ref[R * k : R * (k + 1)] = part


def last_block(recv_ref, both_ref, ortho_ref, parts_ref, turned_ref, q_ref, r_ref):
    total = recv_ref[0]
    for k in range(1, 16):
        total = total + recv_ref[k]
    both = both_ref[...]
    cross = lax.dot_general(total[:, :R], both[:, R:], NT, precision=HIGHEST, preferred_element_type=F32)
    schur = total[:, R : R + RZ] - lax.dot_general(cross, cross, NT, precision=HIGHEST, preferred_element_type=F32)
    hi, mid, _ = three_parts(cross)
    wide = jnp.concatenate([hi, hi, mid, mid], axis=1)
    resid = turned_ref[...] - jnp.dot(wide, parts_ref[...], preferred_element_type=F32)
    blocks = [resid[:, 128 * t : 128 * (t + 1)] for t in range(8)]
    scale, columns, blocks = eliminate(schur, blocks)
    index = lax.broadcasted_iota(jnp.int32, (RZ, 128), 0)
    lane = lax.broadcasted_iota(jnp.int32, (RZ, 128), 1)
    upper = jnp.zeros((RZ, 128), F32)
    for k in range(RZ):
        upper = jnp.where((lane == R + k) & (index <= k), columns[k], upper)
    for t in range(8):
        rows = slice(128 * t, 128 * (t + 1))
        q_ref[rows] = jnp.concatenate([ortho_ref[:, rows], blocks[t] * scale], axis=0).T
    row = lax.broadcasted_iota(jnp.int32, (R, R), 0)
    lane = lax.broadcasted_iota(jnp.int32, (R, R), 1)
    r_ref[0:R] = jnp.concatenate([jnp.where(row <= lane, both[:, :R], 0.0), cross.T], axis=1)
    r_ref[R:] = (upper * scale)[:, : R + RZ]


def per_device(solution_core, operator_core, left_interface, right_interface, rhs_left, rhs_core, rhs_right):
    shape = jax.ShapeDtypeStruct
    sol = solution_core.reshape(ROWS, R)
    left = jnp.transpose(left_interface, (1, 2, 0)).reshape(RA * HALF, R)
    hbm = pl.BlockSpec(memory_space=pltpu.HBM)
    own = call(
        join,
        shape((ROWS + RA * HALF, R), BF16),
        in_hbm(sol),
        in_hbm(left),
        scratch=[pltpu.SemaphoreType.DMA((2,))],
        in_specs=[hbm, hbm],
    )
    both = lax.all_gather(own, "rank", axis=0)
    right = jnp.transpose(right_interface, (1, 2, 0)).reshape(RA * RZ, R)
    rank = lax.axis_index("rank").astype(jnp.int32).reshape(1)
    smem = pl.BlockSpec(memory_space=pltpu.SMEM)
    proj, left, early, rhs_term = call(
        project,
        (
            shape((32, 128, R), BF16),
            shape((RA, R, R), BF16),
            shape((32, 128), BF16),
            shape((128, 128), F32),
        ),
        rank,
        both,
        right,
        rhs_left.T,
        jnp.transpose(rhs_core, (0, 2, 1)).reshape(256, 32),
        rhs_right,
        scratch=[pltpu.VMEM(((R + 1) * PITCH, R), F32)],
        flops=1 << 26,
        in_specs=[smem] + [VMEM] * 5,
    )
    proj = jnp.transpose(proj.reshape(32, RA, RZ, R), (3, 0, 1, 2))
    left = jnp.transpose(left, (1, 0, 2))
    applied = jnp.einsum("xijy,cjyb->cxib", operator_core, proj, preferred_element_type=F32).astype(BF16)
    partial_value = jnp.einsum("cxa,cxib->aib", left, applied, preferred_element_type=F32)
    partial_value = jnp.transpose(partial_value, (2, 0, 1)).astype(BF16)
    chunks = shape((4, 128, 128), BF16)
    keep, give = call(pack, (chunks, chunks), rank, partial_value, flops=1 << 24, in_specs=[smem, VMEM])
    everyone = lax.all_gather(give, "rank", axis=0)
    send = call(
        choose,
        shape((8, 160, 128), BF16),
        rank,
        keep,
        everyone,
        early,
        in_specs=[smem, VMEM, VMEM, VMEM],
    )
    recv = lax.all_to_all(send, "mode", split_axis=0, concat_axis=0, tiled=True)
    turned, send, gram = call(
        residual,
        (shape((RZ, ROWS), F32), shape((16, RZ, 128), F32), shape((16, 128), F32)),
        recv,
        rhs_term,
        sol,
        scratch=[pltpu.VMEM(((RZ + 1) * PITCH, 32), F32)],
        flops=1 << 24,
    )
    recv = lax.all_to_all(send, ("mode", "rank"), split_axis=0, concat_axis=0, tiled=True)
    gram = lax.all_gather(gram, "rank", axis=0)
    factor, ortho, parts = call(
        first_block,
        (shape((R, 2 * R), F32), shape((R, ROWS), F32), shape((4 * R, ROWS), BF16)),
        gram,
        sol,
        flops=1 << 32,
    )
    q_core, r_factor = call(
        last_block,
        (shape((ROWS, R + RZ), F32), shape((R + RZ, R + RZ), F32)),
        recv,
        factor,
        ortho,
        parts,
        turned,
        flops=1 << 26,
    )
    return (q_core.reshape(HALF, 32, R + RZ), r_factor)


def solution(mesh):
    in_specs = (
        P(("sys", "rank"), "mode", None),
        P("sys", "rank", "mode", None),
        P("sys", None, "rank"),
        P("sys", None, None),
        P(("sys", "rank"), None),
        P("sys", "mode", None),
        P("sys", None),
    )
    out_specs = (P(("sys", "rank"), "mode", None), P("sys", None))
    return jax.shard_map(per_device, mesh=mesh, in_specs=in_specs, out_specs=out_specs, check_vma=False)
```

```python
import jax
import jax.numpy as jnp
from jax import lax
from jax.experimental import pallas as pl
from jax.experimental.pallas import tpu as pltpu
from jax.sharding import PartitionSpec as P

INTERPRET = False
F32 = jnp.float32
BF16 = jnp.bfloat16
HIGHEST = lax.Precision.HIGHEST

R = 64
RZ = 16
RA = 8
HALF = 32
PITCH = 36
ROWS = 1024
NT = (((1,), (1,)), ((), ()))
TN = (((0,), (0,)), ((), ()))


VMEM = pl.BlockSpec(memory_space=pltpu.VMEM)


def call(body, outs, *args, scratch=(), flops=0, in_specs=None):
    return pl.pallas_call(
        body,
        out_shape=outs,
        in_specs=in_specs or [VMEM] * len(args),
        out_specs=jax.tree.map(lambda _: VMEM, outs),
        scratch_shapes=scratch,
        interpret=INTERPRET,
        compiler_params=pltpu.CompilerParams(vmem_limit_bytes=12 << 20),
        cost_estimate=pl.CostEstimate(flops=flops, bytes_accessed=1 << 20, transcendentals=0),
    )(*args)


def in_hbm(x):
    return x if INTERPRET else pltpu.with_memory_space_constraint(x, pltpu.HBM)


def three_parts(x):
    hi = x.astype(BF16)
    rest = x - hi.astype(F32)
    mid = rest.astype(BF16)
    return hi, mid, (rest - mid.astype(F32)).astype(BF16)


def join(sol_ref, left_ref, out_ref, sem):
    copies = [
        pltpu.make_async_copy(sol_ref, out_ref.at[0:ROWS], sem.at[0]),
        pltpu.make_async_copy(left_ref, out_ref.at[ROWS : ROWS + RA * HALF], sem.at[1]),
    ]
    for copy in copies:
        copy.start()
    for copy in copies:
        copy.wait()


def project(rank_ref, both_ref, right_ref, rhs_left_ref, rhs_core_ref, rhs_right_ref, proj_ref, left_ref, gram_ref, rhs_ref, sol_ref):
    for c in range(R):
        own = HALF * (c % HALF)
        sol_ref[PITCH * c : PITCH * c + 32] = both_ref[c // HALF, own : own + 32].astype(F32)
    right = right_ref[...]
    for j in range(32):
        rows = sol_ref[pl.ds(j, R, stride=PITCH), :].astype(BF16)
        proj_ref[j] = lax.dot_general(right, rows, NT, preferred_element_type=F32).astype(BF16)
    for x in range(RA):
        for r in range(2):
            left_ref[x, HALF * r : HALF * (r + 1)] = both_ref[r, ROWS + HALF * x : ROWS + HALF * (x + 1)]
    gram = jnp.zeros((R, R), F32)
    for r in range(2):
        s = both_ref[r, 0:ROWS]
        gram = gram + lax.dot_general(s, s, TN, preferred_element_type=F32)
    row = lax.broadcasted_iota(jnp.int32, (HALF, HALF), 0)
    lane = lax.broadcasted_iota(jnp.int32, (HALF, HALF), 1)
    corner = gram[HALF:, HALF:]
    half = jnp.where(rank_ref[0] == 0, jnp.where(row >= lane, gram[:HALF, :HALF], corner), gram[HALF:, :HALF])
    half = jnp.concatenate([half[8 * k : 8 * (k + 1)] for k in range(4)], axis=1)
    diagonal = jnp.sum(jnp.where(row == lane, corner, 0.0), axis=0, keepdims=True)
    diagonal = jnp.broadcast_to(jnp.concatenate([diagonal] * 4, axis=1), (8, 128))
    row = lax.broadcasted_iota(jnp.int32, (8, 128), 0)
    parts = [part.astype(F32) for part in three_parts(half)]
    tail = jnp.zeros((8, 128), F32)
    for p, part in enumerate(three_parts(diagonal)):
        tail = jnp.where(row == p, part.astype(F32), tail)
    gram_ref[...] = jnp.concatenate([*parts, tail], axis=0).astype(BF16)
    turned = jnp.concatenate([rhs_right_ref[...].astype(F32).T] * 8, axis=1)
    turned = jnp.broadcast_to(turned[:, None, :], (16, 16, 128)).reshape(256, 128)
    row = lax.broadcasted_iota(jnp.int32, (256, 128), 0) & 15
    lane = lax.broadcasted_iota(jnp.int32, (256, 128), 1) >> 4
    spread = jnp.concatenate([jnp.where(row == lane + 8 * h, turned, 0.0) for h in range(2)], axis=1).astype(BF16)
    inner = jnp.dot(spread, rhs_core_ref[...], preferred_element_type=F32)
    inner = jnp.concatenate([inner[RZ * b : RZ * (b + 1)] for b in range(RZ)], axis=1)
    stacked = jnp.concatenate(three_parts(inner), axis=0)
    outer = rhs_left_ref[...].astype(F32).T.astype(BF16)
    total = jnp.dot(jnp.concatenate([outer] * 3, axis=1), stacked, preferred_element_type=F32)
    for g in range(4):
        rhs_ref[HALF * g : HALF * (g + 1)] = total[:, 128 * g : 128 * (g + 1)]


def pack(rank_ref, part_ref, keep_ref, give_ref):
    rank = rank_ref[0]
    for out_ref, half in ((keep_ref, rank), (give_ref, 1 - rank)):
        rows = pl.ds(pl.multiple_of(HALF * half, HALF), HALF)
        for g in range(4):
            four = [part_ref[4 * g + k, rows, :].astype(F32) for k in range(4)]
            for q in range(4):
                piece = jnp.concatenate([x[:, 32 * q : 32 * (q + 1)] for x in four], axis=1)
                out_ref[q, HALF * g : HALF * (g + 1)] = piece.astype(BF16)


def choose(rank_ref, keep_ref, every_ref, gram_ref, out_ref):
    rank = rank_ref[0]
    gram = gram_ref[...]
    for q in range(4):
        out_ref[4 * rank + q, 0:128] = keep_ref[q]
        out_ref[4 - 4 * rank + q, 0:128] = every_ref[1 - rank, q]
    for k in range(8):
        out_ref[k, 128:160] = gram


def residual(recv_ref, rhs_ref, sol_ref, turned_ref, send_ref, gram_ref, rows_ref):
    total = recv_ref[0].astype(F32)
    for m in range(1, 8):
        total = total + recv_ref[m].astype(F32)
    gram_ref[0:8] = total[128:136] + total[136:144] + total[144:152]
    gram_ref[8:16] = jnp.broadcast_to(total[152:153] + total[153:154] + total[154:155], (8, 128))
    resid = rhs_ref[...] - total[0:128]
    for k in range(4):
        shifted = resid if k == 0 else pltpu.roll(resid, 128 - 32 * k, 1)
        for g in range(4):
            b = 4 * g + k
            rows_ref[PITCH * b : PITCH * b + HALF] = shifted[HALF * g : HALF * (g + 1), :32]
    for t in range(8):
        four = [rows_ref[pl.ds(4 * t + s, RZ, stride=PITCH), :] for s in range(4)]
        turned_ref[:, 128 * t : 128 * (t + 1)] = jnp.concatenate(four, axis=1)
    turned = turned_ref[...]
    stacked = jnp.concatenate(three_parts(turned), axis=0)
    cross = jnp.dot(stacked, sol_ref[...], preferred_element_type=F32)
    cross = cross[0:16] + cross[16:32] + cross[32:48]
    pairs = lax.dot_general(stacked, stacked, NT, preferred_element_type=F32)
    own = pairs[0:16, 16:32] + pairs[0:16, 32:48] + pairs[16:32, 16:32] + pairs[16:32, 0:16] + pairs[32:48, 0:16]
    own = own + pairs[0:16, 0:16]
    row = jnp.concatenate([cross, own, jnp.zeros((RZ, 48), F32)], axis=1)
    for k in range(16):
        send_ref[k] = row


def eliminate(square, blocks):
    columns = [jnp.broadcast_to(square[:, k : k + 1], (RZ, 128)) for k in range(RZ)]
    index = lax.broadcasted_iota(jnp.int32, (RZ, 128), 0)
    pivots = jnp.zeros((RZ, 128), F32)
    for k in range(RZ):
        pivots = jnp.where(index == k, columns[k], pivots)
        factor = jnp.where(index > k, columns[k] / columns[k][k : k + 1], 0.0)
        for j in range(k + 1, RZ):
            columns[j] = columns[j] - factor * columns[j][k : k + 1]
        blocks = [x - factor * x[k : k + 1] for x in blocks]
    return lax.rsqrt(pivots), columns, blocks


def first_block(gram_ref, sol_ref, both_ref, ortho_ref, parts_ref):
    row = lax.broadcasted_iota(jnp.int32, (HALF, HALF), 0)
    lane = lax.broadcasted_iota(jnp.int32, (HALF, HALF), 1)
    halves = [jnp.concatenate([gram_ref[r, 0:8, 32 * k : 32 * (k + 1)] for k in range(4)], axis=0) for r in range(2)]
    mirror = halves[0].T
    first = jnp.where(row >= lane, halves[0], mirror)
    corner = jnp.where(row < lane, halves[0], mirror)
    corner = jnp.where(row == lane, gram_ref[0, 8:9, 0:32], corner)
    eye = (lax.broadcasted_iota(jnp.int32, (R, R), 0) == lax.broadcasted_iota(jnp.int32, (R, R), 1)).astype(F32)
    gram = jnp.concatenate(
        [jnp.concatenate([first, halves[1].T], axis=1), jnp.concatenate([halves[1], corner], axis=1)], axis=0
    )
    rest = jnp.concatenate([gram, eye], axis=1)
    done = []
    for k in range(4):
        scale, _, (top,) = eliminate(rest[0:RZ, RZ * k : RZ * (k + 1)], [rest[0:RZ]])
        top = top * scale
        done.append(top)
        if k < 3:
            across = top[:, RZ * (k + 1) : R]
            rest = rest[RZ:] - lax.dot_general(across, top, TN, precision=HIGHEST, preferred_element_type=F32)
    both = jnp.concatenate(done, axis=0)
    both_ref[...] = both
    stacked = jnp.concatenate(three_parts(both[:, R:]), axis=0)
    ortho = lax.dot_general(stacked, sol_ref[...], NT, preferred_element_type=F32)
    ortho = ortho[0:R] + ortho[R : 2 * R] + ortho[2 * R :]
    ortho_ref[...] = ortho
    hi, mid, _ = three_parts(ortho)
    for k, part in enumerate((hi, mid, hi, mid)):
        parts_ref[R * k : R * (k + 1)] = part


def last_block(recv_ref, both_ref, ortho_ref, parts_ref, turned_ref, q_ref, r_ref):
    total = recv_ref[0]
    for k in range(1, 16):
        total = total + recv_ref[k]
    both = both_ref[...]
    cross = lax.dot_general(total[:, :R], both[:, R:], NT, precision=HIGHEST, preferred_element_type=F32)
    schur = total[:, R : R + RZ] - lax.dot_general(cross, cross, NT, precision=HIGHEST, preferred_element_type=F32)
    hi, mid, _ = three_parts(cross)
    wide = jnp.concatenate([hi, hi, mid, mid], axis=1)
    resid = turned_ref[...] - jnp.dot(wide, parts_ref[...], preferred_element_type=F32)
    blocks = [resid[:, 128 * t : 128 * (t + 1)] for t in range(8)]
    scale, columns, blocks = eliminate(schur, blocks)
    index = lax.broadcasted_iota(jnp.int32, (RZ, 128), 0)
    lane = lax.broadcasted_iota(jnp.int32, (RZ, 128), 1)
    upper = jnp.zeros((RZ, 128), F32)
    for k in range(RZ):
        upper = jnp.where((lane == R + k) & (index <= k), columns[k], upper)
    for t in range(8):
        rows = slice(128 * t, 128 * (t + 1))
        q_ref[rows] = jnp.concatenate([ortho_ref[:, rows], blocks[t] * scale], axis=0).T
    row = lax.broadcasted_iota(jnp.int32, (R, R), 0)
    lane = lax.broadcasted_iota(jnp.int32, (R, R), 1)
    r_ref[0:R] = jnp.concatenate([jnp.where(row <= lane, both[:, :R], 0.0), cross.T], axis=1)
    r_ref[R:] = (upper * scale)[:, : R + RZ]


def per_device(solution_core, operator_core, left_interface, right_interface, rhs_left, rhs_core, rhs_right):
    shape = jax.ShapeDtypeStruct
    sol = solution_core.reshape(ROWS, R)
    left = jnp.transpose(left_interface, (1, 2, 0)).reshape(RA * HALF, R)
    hbm = pl.BlockSpec(memory_space=pltpu.HBM)
    own = call(
        join,
        shape((ROWS + RA * HALF, R), BF16),
        in_hbm(sol),
        in_hbm(left),
        scratch=[pltpu.SemaphoreType.DMA((2,))],
        in_specs=[hbm, hbm],
    )
    both = lax.all_gather(own, "rank", axis=0)
    right = jnp.transpose(right_interface, (1, 2, 0)).reshape(RA * RZ, R)
    rank = lax.axis_index("rank").astype(jnp.int32).reshape(1)
    smem = pl.BlockSpec(memory_space=pltpu.SMEM)
    proj, left, early, rhs_term = call(
        project,
        (
            shape((32, 128, R), BF16),
            shape((RA, R, R), BF16),
            shape((32, 128), BF16),
            shape((128, 128), F32),
        ),
        rank,
        both,
        right,
        rhs_left.T,
        jnp.transpose(rhs_core, (0, 2, 1)).reshape(256, 32),
        rhs_right,
        scratch=[pltpu.VMEM(((R + 1) * PITCH, R), F32)],
        flops=1 << 26,
        in_specs=[smem] + [VMEM] * 5,
    )
    proj = jnp.transpose(proj.reshape(32, RA, RZ, R), (3, 0, 1, 2))
    left = jnp.transpose(left, (1, 0, 2))
    applied = jnp.einsum("xijy,cjyb->cxib", operator_core, proj, preferred_element_type=F32).astype(BF16)
    partial_value = jnp.einsum("cxa,cxib->aib", left, applied, preferred_element_type=F32)
    partial_value = jnp.transpose(partial_value, (2, 0, 1)).astype(BF16)
    chunks = shape((4, 128, 128), BF16)
    keep, give = call(pack, (chunks, chunks), rank, partial_value, flops=1 << 24, in_specs=[smem, VMEM])
    everyone = lax.all_gather(give, "rank", axis=0)
    send = call(
        choose,
        shape((8, 160, 128), BF16),
        rank,
        keep,
        everyone,
        early,
        in_specs=[smem, VMEM, VMEM, VMEM],
    )
    recv = lax.all_to_all(send, "mode", split_axis=0, concat_axis=0, tiled=True)
    turned, send, gram = call(
        residual,
        (shape((RZ, ROWS), F32), shape((16, RZ, 128), F32), shape((16, 128), F32)),
        recv,
        rhs_term,
        sol,
        scratch=[pltpu.VMEM(((RZ + 1) * PITCH, 32), F32)],
        flops=1 << 24,
    )
    recv = lax.all_to_all(send, ("mode", "rank"), split_axis=0, concat_axis=0, tiled=True)
    gram = lax.all_gather(gram, "rank", axis=0)
    factor, ortho, parts = call(
        first_block,
        (shape((R, 2 * R), F32), shape((R, ROWS), F32), shape((4 * R, ROWS), BF16)),
        gram,
        sol,
        flops=1 << 32,
    )
    q_core, r_factor = call(
        last_block,
        (shape((ROWS, R + RZ), F32), shape((R + RZ, R + RZ), F32)),
        recv,
        factor,
        ortho,
        parts,
        turned,
        flops=1 << 26,
    )
    return (q_core.reshape(HALF, 32, R + RZ), r_factor)


def solution(mesh):
    in_specs = (
        P(("sys", "rank"), "mode", None),
        P("sys", "rank", "mode", None),
        P("sys", None, "rank"),
        P("sys", None, None),
        P(("sys", "rank"), None),
        P("sys", "mode", None),
        P("sys", None),
    )
    out_specs = (P(("sys", "rank"), "mode", None), P("sys", None))
    return jax.shard_map(per_device, mesh=mesh, in_specs=in_specs, out_specs=out_specs, check_vma=False)
```
